32 devices in a mesh: space: 8 (over z, y), tm: 4 (over x, core).
Axes of the slice: x: 2, y: 2, z: 4, core: 2. Of those that a mesh axis runs over, the one named last changes fastest.
Arguments:
- precip: float32 [512, 48, 2048], P('tm', 'space'), may hold values from 0.0001 to 0.01
Outputs:
- totals: float32 [48, 2048, 512], P(None, 'space', 'tm')
The draws below stay inside these ranges and needn't reach their ends.
All inputs are finite; a program needn't handle non-finite values.
Results may differ from the reference program's by a relative error of at most 0.00005.
Values sent between devices are 32-bit elements; how exact they have to be, the bound alone decides.
A program may use at most 64 MiB of HBM per device.

```python
import math
import jax
import jax.numpy as jnp

LON = 2048
DAYS = 512
LAT = 48


def steps_of(rng, dims, split, least, high):
    def one(position, blocks):
        steps = jax.random.uniform(jax.random.fold_in(jax.random.fold_in(rng, 6), position), (blocks,), jnp.float32, least / len(split), high / len(split))
        return jnp.repeat(jnp.exp(steps), dims[position] // blocks).reshape((-1,) + (1,) * (len(dims) - position - 1))

    factor_of = one(*split[0])
    for cut in split[1:]:
        factor_of = factor_of * one(*cut)
    return factor_of


def setup_inputs(seed: int = 0) -> dict:
    key_list = jax.random.split(jax.random.key(seed), 2)
    precip = jnp.clip(jnp.exp(math.log(0.01) - 4.6051702 * jax.random.uniform(key_list[0], (DAYS, LAT, LON), jnp.float32) ** steps_of(key_list[0], (DAYS, LAT, LON), ((0, 4), (1, 8)), -0.2, 0.2)), 0.0001, 0.01)
    return {"precip": precip}


def reference(precip):
    running = jnp.cumsum(precip, axis=0)
    return jnp.transpose(running, (1, 2, 0))
```

```python
import functools

import jax
import jax.numpy as jnp
from jax import lax
from jax.experimental import pallas as pl
from jax.experimental.pallas import tpu as pltpu
from jax.sharding import PartitionSpec as P

MESH = pl.DeviceIdType.MESH
HEAD = 8
CHUNKS = 2
FIRST = 3


def flip(place, mask):
    value, bit = 0, 1
    while bit <= mask:
        value = value + ((place // bit + mask // bit) % 2) * bit
        bit *= 2
    return value + (place // bit) * bit


def peer_at(place, step, size):
    if size & (size - 1) == 0:
        return flip(place, step)
    return lax.rem(place + step, size)


def source_at(place, step, size):
    if size & (size - 1) == 0:
        return flip(place, step)
    return lax.rem(place + size - step, size)


def kernel(spaces, times, chunks, x_ref, out_ref, held, arrived, tot, tots, ones,
           load_sem, main_send, main_recv, head_send, head_recv, tot_send, tot_recv):
    lat, days, lon = x_ref.shape
    block = lon // spaces
    part = lat // chunks
    me = lax.axis_index("space")
    when = lax.axis_index("tm")

    loads = [pltpu.make_async_copy(x_ref.at[a], held.at[a], load_sem.at[a]) for a in range(lat)]
    barrier = pltpu.get_barrier_semaphore()
    for step in range(1, spaces):
        pl.semaphore_signal(barrier, inc=1, device_id={"space": peer_at(me, step, spaces)}, device_id_type=MESH)
    for step in range(1, times):
        pl.semaphore_signal(barrier, inc=1, device_id={"tm": lax.rem(when + step, times)}, device_id_type=MESH)
    for load in loads:
        load.start()
    pl.semaphore_wait(barrier, spaces - 1 + times - 1)

    def columns(step):
        peer = peer_at(me, step, spaces)
        return peer, pl.ds(pl.multiple_of(peer * block, block), block)

    def main(step, c):
        peer, cols = columns(step)
        return pltpu.make_async_remote_copy(
            src_ref=x_ref.at[pl.ds(c * part, part), pl.ds(HEAD, days - HEAD), cols],
            dst_ref=arrived.at[step - 1, pl.ds(c * part, part), pl.ds(HEAD, days - HEAD)],
            send_sem=main_send.at[step - 1, c],
            recv_sem=main_recv.at[step - 1, c],
            device_id={"space": peer},
            device_id_type=MESH,
        )

    def head(step):
        peer, cols = columns(step)
        return pltpu.make_async_remote_copy(
            src_ref=held.at[:, pl.ds(0, HEAD), cols],
            dst_ref=arrived.at[step - 1, :, pl.ds(0, HEAD)],
            send_sem=head_send.at[step - 1],
            recv_sem=head_recv.at[step - 1],
            device_id={"space": peer},
            device_id_type=MESH,
        )

    def total(step):
        return pltpu.make_async_remote_copy(
            src_ref=tot,
            dst_ref=tots.at[step - 1],
            send_sem=tot_send.at[step - 1],
            recv_sem=tot_recv.at[step - 1],
            device_id={"tm": lax.rem(when + step, times)},
            device_id_type=MESH,
        )

    first = min(FIRST, spaces - 1)
    for step in range(1, first + 1):
        for c in range(chunks):
            main(step, c).start()

    for a in range(lat):
        loads[a].wait()
        tot[a] = jnp.sum(held[a], axis=0, keepdims=True)
    position = lax.broadcasted_iota(jnp.int32, (days, days), 0)
    later = lax.broadcasted_iota(jnp.int32, (days, days), 1)
    ones[...] = (position <= later).astype(jnp.float32)
    for step in range(1, times):
        total(step).start()
    for step in range(1, times):
        total(step).wait_recv()
    for a in range(lat):
        carry = jnp.zeros((1, lon), jnp.float32)
        for step in range(1, times):
            earlier = jnp.where(when >= step, 1.0, 0.0)
            carry = carry + tots[step - 1, a] * earlier
        held[a, 0:1, :] = held[a, 0:1, :] + carry

    def prefix(x):
        return lax.dot_general(
            x.T, ones[...], (((1,), (0,)), ((), ())),
            precision=lax.Precision.HIGHEST, preferred_element_type=jnp.float32,
        )

    for step in range(1, spaces):
        head(step).start()
    for step in range(first + 1, spaces):
        for c in range(chunks):
            main(step, c).start()

    mine = pl.ds(pl.multiple_of(me * block, block), block)

    @pl.loop(0, lat)
    def _(a):
        out_ref[me * lat + a] = prefix(held[a, :, mine])

    for step in range(1, spaces):
        source = source_at(me, step, spaces)
        head(step).wait_recv()
        for c in range(chunks):
            main(step, c).wait_recv()

            @pl.loop(c * part, (c + 1) * part)
            def _(a):
                out_ref[source * lat + a] = prefix(arrived[step - 1, a])

    for step in range(1, times):
        total(step).wait_send()
    for step in range(1, spaces):
        head(step).wait_send()
        for c in range(chunks):
            main(step, c).wait_send()


def direct(spaces, times, precip):
    days, lat, lon = precip.shape
    chunks = CHUNKS if lat % CHUNKS == 0 else 1
    block = lon // spaces
    rows = jnp.transpose(precip, (1, 0, 2))
    dma = pltpu.SemaphoreType.DMA
    return pl.pallas_call(
        functools.partial(kernel, spaces, times, chunks),
        out_shape=jax.ShapeDtypeStruct((lat * spaces, block, days), jnp.float32),
        in_specs=[pl.BlockSpec(memory_space=pltpu.HBM)],
        out_specs=pl.BlockSpec(memory_space=pltpu.VMEM),
        scratch_shapes=[
            pltpu.VMEM((lat, days, lon), jnp.float32),
            pltpu.VMEM((spaces - 1, lat, days, block), jnp.float32),
            pltpu.VMEM((lat, 1, lon), jnp.float32),
            pltpu.VMEM((times - 1, lat, 1, lon), jnp.float32),
            pltpu.VMEM((days, days), jnp.float32),
            dma((lat,)),
            dma((spaces - 1, chunks)),
            dma((spaces - 1, chunks)),
            dma((spaces - 1,)),
            dma((spaces - 1,)),
            dma((times - 1,)),
            dma((times - 1,)),
        ],
        compiler_params=pltpu.CompilerParams(
            collective_id=0, has_side_effects=True, vmem_limit_bytes=55 * 2**20
        ),
        name="rechunk",
    )(rows)


def plain(precip):
    days = precip.shape[0]
    position = lax.broadcasted_iota(jnp.int32, (days, days), 0)
    later = lax.broadcasted_iota(jnp.int32, (days, days), 1)
    ones = (position <= later).astype(jnp.float32)
    source = lax.all_to_all(precip, "space", split_axis=2, concat_axis=1, tiled=True)
    pixel_major = jnp.transpose(source, (1, 2, 0))
    running = jnp.dot(
        pixel_major, ones, precision=lax.Precision.HIGHEST, preferred_element_type=jnp.float32
    )
    last = lax.all_gather(running[:, :, -1], "tm")
    place = lax.broadcasted_iota(jnp.int32, last.shape, 0)
    carried = jnp.sum(jnp.where(place < lax.axis_index("tm"), last, 0.0), axis=0)
    return running + carried[:, :, None]


def solution(mesh):
    spaces, times = mesh.shape["space"], mesh.shape["tm"]

    def per_device(precip):
        days, _, lon = precip.shape
        tiled = lon % (spaces * 128) == 0 and days % 128 == 0
        if tiled and spaces > 1 and times > 1:
            return direct(spaces, times, precip)
        return plain(precip)

    return jax.shard_map(
        per_device,
        mesh=mesh,
        in_specs=(P("tm", "space", None),),
        out_specs=P(None, "space", "tm"),
        check_vma=False,
    )
```

```python
import functools

import jax
import jax.numpy as jnp
from jax import lax
from jax.experimental import pallas as pl
from jax.experimental.pallas import tpu as pltpu
from jax.sharding import PartitionSpec as P

MESH = pl.DeviceIdType.MESH
HEAD = 8
CHUNKS = 2
FIRST = 3


def turns_of(spaces):
    near = list(range(1, spaces))
    if spaces & (spaces - 1) or spaces < 4:
        return near, near
    return near, [step ^ 1 for step in near[1:]] + [1]


def flip(place, mask, size):
    value, bit = 0, 1
    while bit < size:
        value = value + ((place // bit + mask // bit) % 2) * bit
        bit *= 2
    return value


def peer_at(place, step, size):
    if size & (size - 1) == 0:
        return flip(place, step, size)
    return lax.rem(place + step, size)


def source_at(place, step, size):
    if size & (size - 1) == 0:
        return flip(place, step, size)
    return lax.rem(place + size - step, size)


def kernel(spaces, times, chunks, x_ref, out_ref, held, arrived, tot, tots, ones,
           load_sem, main_send, main_recv, head_send, head_recv, tot_send, tot_recv):
    lat, days, lon = x_ref.shape
    block = lon // spaces
    part = lat // chunks
    me = lax.axis_index("space")
    when = lax.axis_index("tm")

    loads = [pltpu.make_async_copy(x_ref.at[a], held.at[a], load_sem.at[a]) for a in range(lat)]
    barrier = pltpu.get_barrier_semaphore()
    for step in range(1, spaces):
        pl.semaphore_signal(barrier, inc=1, device_id={"space": peer_at(me, step, spaces)}, device_id_type=MESH)
    for step in range(1, times):
        pl.semaphore_signal(barrier, inc=1, device_id={"tm": lax.rem(when + step, times)}, device_id_type=MESH)
    for load in loads:
        load.start()
    pl.semaphore_wait(barrier, spaces - 1 + times - 1)

    def columns(step):
        peer = peer_at(me, step, spaces)
        return peer, pl.ds(pl.multiple_of(peer * block, block), block)

    def main(step, c):
        peer, cols = columns(step)
        return pltpu.make_async_remote_copy(
            src_ref=x_ref.at[pl.ds(c * part, part), pl.ds(HEAD, days - HEAD), cols],
            dst_ref=arrived.at[step - 1, pl.ds(c * part, part), pl.ds(HEAD, days - HEAD)],
            send_sem=main_send.at[step - 1, c],
            recv_sem=main_recv.at[step - 1, c],
            device_id={"space": peer},
            device_id_type=MESH,
        )

    def head(step):
        peer, cols = columns(step)
        return pltpu.make_async_remote_copy(
            src_ref=held.at[:, pl.ds(0, HEAD), cols],
            dst_ref=arrived.at[step - 1, :, pl.ds(0, HEAD)],
            send_sem=head_send.at[step - 1],
            recv_sem=head_recv.at[step - 1],
            device_id={"space": peer},
            device_id_type=MESH,
        )

    def total(step):
        return pltpu.make_async_remote_copy(
            src_ref=tot,
            dst_ref=tots.at[step - 1],
            send_sem=tot_send.at[step - 1],
            recv_sem=tot_recv.at[step - 1],
            device_id={"tm": lax.rem(when + step, times)},
            device_id_type=MESH,
        )

    first = min(FIRST, spaces - 1)
    even, odd = turns_of(spaces)
    turns = [a if a == b else jnp.where(when % 2 == 0, a, b) for a, b in zip(even, odd)]
    for step in turns[:first]:
        for c in range(chunks):
            main(step, c).start()

    for a in range(lat):
        loads[a].wait()
        tot[a] = jnp.sum(held[a], axis=0, keepdims=True)
    position = lax.broadcasted_iota(jnp.int32, (days, days), 0)
    later = lax.broadcasted_iota(jnp.int32, (days, days), 1)
    ones[...] = (position <= later).astype(jnp.float32)
    for step in range(1, times):
        total(step).start()
    for step in range(1, times):
        total(step).wait_recv()
    for a in range(lat):
        carry = jnp.zeros((1, lon), jnp.float32)
        for step in range(1, times):
            earlier = jnp.where(when >= step, 1.0, 0.0)
            carry = carry + tots[step - 1, a] * earlier
        held[a, 0:1, :] = held[a, 0:1, :] + carry

    def prefix(x):
        return lax.dot_general(
            x.T, ones[...], (((1,), (0,)), ((), ())),
            precision=lax.Precision.HIGHEST, preferred_element_type=jnp.float32,
        )

    for step in turns:
        head(step).start()
    for step in turns[first:]:
        for c in range(chunks):
            main(step, c).start()

    mine = pl.ds(pl.multiple_of(me * block, block), block)

    @pl.loop(0, lat)
    def _(a):
        out_ref[me * lat + a] = prefix(held[a, :, mine])

    for step in turns:
        source = source_at(me, step, spaces)
        head(step).wait_recv()
        for c in range(chunks):
            main(step, c).wait_recv()

            @pl.loop(c * part, (c + 1) * part)
            def _(a):
                out_ref[source * lat + a] = prefix(arrived[step - 1, a])

    for step in range(1, times):
        total(step).wait_send()
    for step in range(1, spaces):
        head(step).wait_send()
        for c in range(chunks):
            main(step, c).wait_send()


def direct(spaces, times, precip):
    days, lat, lon = precip.shape
    chunks = CHUNKS if lat % CHUNKS == 0 else 1
    block = lon // spaces
    rows = jnp.transpose(precip, (1, 0, 2))
    dma = pltpu.SemaphoreType.DMA
    return pl.pallas_call(
        functools.partial(kernel, spaces, times, chunks),
        out_shape=jax.ShapeDtypeStruct((lat * spaces, block, days), jnp.float32),
        in_specs=[pl.BlockSpec(memory_space=pltpu.HBM)],
        out_specs=pl.BlockSpec(memory_space=pltpu.VMEM),
        scratch_shapes=[
            pltpu.VMEM((lat, days, lon), jnp.float32),
            pltpu.VMEM((spaces - 1, lat, days, block), jnp.float32),
            pltpu.VMEM((lat, 1, lon), jnp.float32),
            pltpu.VMEM((times - 1, lat, 1, lon), jnp.float32),
            pltpu.VMEM((days, days), jnp.float32),
            dma((lat,)),
            dma((spaces - 1, chunks)),
            dma((spaces - 1, chunks)),
            dma((spaces - 1,)),
            dma((spaces - 1,)),
            dma((times - 1,)),
            dma((times - 1,)),
        ],
        compiler_params=pltpu.CompilerParams(
            collective_id=0, has_side_effects=True, vmem_limit_bytes=46 * 2**20
        ),
        name="rechunk",
    )(rows)


def plain(precip):
    days = precip.shape[0]
    position = lax.broadcasted_iota(jnp.int32, (days, days), 0)
    later = lax.broadcasted_iota(jnp.int32, (days, days), 1)
    ones = (position <= later).astype(jnp.float32)
    source = lax.all_to_all(precip, "space", split_axis=2, concat_axis=1, tiled=True)
    pixel_major = jnp.transpose(source, (1, 2, 0))
    running = jnp.dot(
        pixel_major, ones, precision=lax.Precision.HIGHEST, preferred_element_type=jnp.float32
    )
    last = lax.all_gather(running[:, :, -1], "tm")
    place = lax.broadcasted_iota(jnp.int32, last.shape, 0)
    carried = jnp.sum(jnp.where(place < lax.axis_index("tm"), last, 0.0), axis=0)
    return running + carried[:, :, None]


def solution(mesh):
    spaces, times = mesh.shape["space"], mesh.shape["tm"]

    def per_device(precip):
        days, _, lon = precip.shape
        tiled = lon % (spaces * 128) == 0 and days % 128 == 0
        if tiled and spaces > 1 and times > 1:
            return direct(spaces, times, precip)
        return plain(precip)

    return jax.shard_map(
        per_device,
        mesh=mesh,
        in_specs=(P("tm", "space", None),),
        out_specs=P(None, "space", "tm"),
        check_vma=False,
    )
```
